128 devices in a mesh: dev: 128 (over x, z, y, core).
Axes of the slice: x: 4, y: 4, z: 4, core: 2. Of those that a mesh axis runs over, the one named last changes fastest.
Arguments:
- pixels: bfloat16 [128, 256, 16], P('dev'), may hold values from -6 to 6
- embed_w: bfloat16 [128, 16, 8192], P('dev'), may hold values from -1.5 to 1.5
- var_embed: bfloat16 [128, 8192], P('dev'), may hold values from -3 to 3
- key_w: bfloat16 [8192, 8192], P('dev'), may hold values from -0.0625 to 0.0625
- query: float32 [8192], replicated, may hold values from -500 to 500
- value_t: bfloat16 [8192, 8192], P('dev'), may hold values from -0.0625 to 0.0625
- out_w: bfloat16 [8192, 8192], P('dev'), may hold values from -0.0625 to 0.0625
Outputs:
- mixed: bfloat16 [256, 8192], P('dev')
The draws below stay inside these ranges and needn't reach their ends.
All inputs are finite; a program needn't handle non-finite values.
Results may differ from the reference program's by a relative error of at most 0.012.
The reference program's roundings to bfloat16 on the way (of `embed`, `attn`, `pooled` and `heads`) count: a program that leaves them out, or rounds other values in their place, can miss the bound.
Values may be sent and summed in bfloat16 or wider, within the bound.
A program may use at most 64 MiB of HBM per device.

```python
import jax
import jax.numpy as jnp
from jax import lax

D = 8192
HEADS = 64
HD = 128
P_SIZE = 16
V = 91
TOK_DEV = 2
VSLOT = 128
TOKENS = 256
N_DEV = 128


def draw_query(key, part):
    first, second = jax.random.split(jax.random.fold_in(key, 17))
    base = jnp.clip(jax.random.normal(first, (HEADS, HD), jnp.float32), -5.0, 5.0)
    scales = jnp.exp(jax.random.uniform(second, (HEADS, 1), jnp.float32, jnp.log(0.5), jnp.log(3.0)))
    return (base * scales).reshape(HEADS * HD)


def steps_of(key, shape, cuts, low, largest):
    gain = 1.0
    for dim, shards_of in cuts:
        heights = jax.random.uniform(jax.random.fold_in(jax.random.fold_in(key, 6), dim), (shards_of,), jnp.float32, low / len(cuts), largest / len(cuts))
        gain = gain * jnp.repeat(jnp.exp(heights), shape[dim] // shards_of).reshape((-1,) + (1,) * (len(shape) - 1 - dim))
    return gain


def bell_draw(own_key, shape, deviation, reach, shards=(), held_as=jnp.bfloat16):
    array = deviation * jax.random.normal(own_key, shape, jnp.float32)
    if shards:
        array = array * steps_of(own_key, shape, shards, -0.22, 0.18)
    return jnp.clip(array, -reach, reach).astype(held_as)


def setup_inputs(seed: int = 0) -> dict:
    key_of = jax.random.split(jax.random.key(seed), 8)
    pixels = bell_draw(key_of[0], (VSLOT, TOKENS, P_SIZE), 1.0, 6.0, ((0, 128),))
    embed_w = bell_draw(key_of[1], (VSLOT, P_SIZE, D), P_SIZE ** -0.5, 1.5, ((0, 128),))
    var_embed = bell_draw(key_of[2], (VSLOT, D), 0.5, 3.0, ((0, 128),))
    key_w = bell_draw(key_of[3], (D, D), D ** -0.5, 0.0625, ((0, 128),))
    query = draw_query(jax.random.fold_in(key_of[7], 71), 0)
    value_t = bell_draw(key_of[5], (D, D), D ** -0.5, 0.0625, ((0, 128),))
    out_w = bell_draw(key_of[6], (D, D), D ** -0.5, 0.0625, ((0, 128),))
    return {"pixels": pixels, "embed_w": embed_w, "var_embed": var_embed, "key_w": key_w, "query": query, "value_t": value_t, "out_w": out_w}


def reference(pixels, embed_w, var_embed, key_w, query, value_t, out_w):
    query_heads = query.reshape(HEADS, HD)
    keyq = jnp.einsum('dhj,hj->dh', key_w.astype(jnp.float32).reshape(D, HEADS, HD), query_heads, precision=lax.Precision.HIGHEST)
    value_full = value_t.astype(jnp.float32).reshape(HEADS, HD, D)
    live_pixels = pixels[:V].reshape(V, N_DEV, TOK_DEV, P_SIZE).transpose(1, 0, 2, 3)
    live_embed_w = embed_w[:V].astype(jnp.float32)
    live_var = var_embed[:V].astype(jnp.float32)

    def one_block(block):
        embed = jnp.einsum('vtp,vpd->vtd', block.astype(jnp.float32), live_embed_w, precision=lax.Precision.HIGHEST)
        embed = (embed + live_var[:, None, :]).astype(jnp.bfloat16)
        logits = jnp.einsum('vtd,dh->vth', embed.astype(jnp.float32), keyq, precision=lax.Precision.HIGHEST) / jnp.sqrt(jnp.float32(HD))
        row_max = lax.optimization_barrier(jnp.max(logits, axis=0, keepdims=True))
        weights = jnp.exp(logits - row_max)
        attn = (weights / lax.optimization_barrier(jnp.sum(weights, axis=0, keepdims=True))).astype(jnp.bfloat16)
        pooled = jnp.einsum('vth,vtd->thd', attn.astype(jnp.float32), embed.astype(jnp.float32), precision=lax.Precision.HIGHEST).astype(jnp.bfloat16)
        heads = jnp.einsum('thd,hcd->thc', pooled.astype(jnp.float32), value_full, precision=lax.Precision.HIGHEST)
        heads = heads.reshape(TOK_DEV, D).astype(jnp.bfloat16)
        return jnp.dot(heads, out_w, preferred_element_type=jnp.float32).astype(jnp.bfloat16)
    mixed = lax.map(one_block, live_pixels)
    return mixed.reshape(TOKENS, D)
```

```python
import jax
import jax.numpy as jnp
from jax import lax
from jax.experimental import pallas as pl
from jax.experimental.pallas import tpu as pltpu
from jax.sharding import PartitionSpec as P

D = 8192
HEADS = 64
HD = 128
V = 91
MESH = pl.DeviceIdType.MESH
BF = jnp.bfloat16
F32 = jnp.float32
OFFSETS = (0, -1, 1, 2)


def dot(a, b, dims):
    return lax.dot_general(a, b, (dims, ((), ())), preferred_element_type=F32)


def kernel(
    pix_ref,
    ew_ref,
    var_ref,
    kw_ref,
    q_ref,
    vt_ref,
    ow_ref,
    out_ref,
    kw,
    ew,
    vf,
    pixp,
    pixt,
    wpart,
    vpart,
    ppart,
    emb,
    kqs,
    kq,
    eb,
    vs,
    px,
    vt,
    ow,
    lps,
    lpr,
    ls,
    lq,
    lr,
    aw,
    evt,
    at,
    hp,
    hr,
    hg,
    ms,
    mr,
    ob,
    obr,
    loc_sem,
    ssem,
    el_rs,
    vl_rs,
    pl_rs,
    part_rs,
    kl_rs,
    vt_rs,
    ow_rs,
    kag_rs,
    eag_rs,
    pag_rs,
    lp_rs,
    lq_rs,
    lr_rs,
    hr_rs,
    hg_rs,
    mr_rs,
    ob_rs,
):
    me = lax.axis_index("dev")
    x = lax.div(me, 32)
    p = lax.rem(lax.div(me, 2), 16)
    c = lax.rem(me, 2)
    z = lax.div(p, 4)
    y = lax.rem(p, 4)
    s = 2 * x + c
    partner = x * 32 + p * 2 + (1 - c)
    source = x < 3

    def dev(s_, p_):
        return lax.div(s_, 2) * 32 + p_ * 2 + lax.rem(s_, 2)

    def wrap8(v):
        return lax.rem(v + 8, 8)

    def wrap16(v):
        return lax.rem(v + 16, 16)

    pending = []
    counter = [0]

    def send(src, dst, rs, d, like=None):
        number = counter[0]
        counter[0] += 1
        sem = ssem.at[number]
        pltpu.make_async_remote_copy(
            src_ref=src, dst_ref=dst, send_sem=sem, recv_sem=rs, device_id=(d,), device_id_type=MESH
        ).start()
        if like is None:
            pending.append((src, sem))
        return like, number

    def wait(ref, sem):
        pltpu.make_async_copy(ref, ref, sem).wait()

    def drain(pairs):
        for like, number in pairs:
            wait(like(), ssem.at[number])

    barrier = pltpu.get_barrier_semaphore()
    for k in range(1, 8):
        pl.semaphore_signal(barrier, inc=1, device_id=(dev(wrap8(s + k), p),), device_id_type=MESH)
    for k in range(1, 16):
        pl.semaphore_signal(barrier, inc=1, device_id=(dev(s, wrap16(p + k)),), device_id_type=MESH)
    kw_in = pltpu.make_async_copy(kw_ref, kw, loc_sem.at[0])
    kw_in.start()
    ew_in = pltpu.make_async_copy(ew_ref.at[0], ew, loc_sem.at[1])
    ew_in.start()

    pos = lax.broadcasted_iota(jnp.int32, (256, 256), 0)
    tok = lax.broadcasted_iota(jnp.int32, (256, 256), 1)
    want = lax.div(lax.rem(pos, 16), 4) * 64 + lax.div(pos, 16) * 4 + lax.rem(pos, 4)
    perm = jnp.where(tok == want, 1.0, 0.0).astype(BF)
    ordered = dot(perm, pix_ref[0], ((1,), (0,))).astype(BF)
    pixp[...] = ordered
    eye = jnp.where(
        lax.broadcasted_iota(jnp.int32, (16, 16), 0) == lax.broadcasted_iota(jnp.int32, (16, 16), 1), 1.0, 0.0
    ).astype(BF)
    pixt[...] = dot(eye, ordered, ((1,), (1,))).astype(BF)
    for k in range(8):
        vf[k] = var_ref[:, k * 1024 : (k + 1) * 1024].astype(F32)
    eb[:, 7] = jnp.zeros((16, 16, 1024), BF)
    ew_in.wait()
    pl.semaphore_wait(barrier, 22)

    half = pl.multiple_of((1 - c) * 4096, 4096)
    first_sends = []
    line_ids = [wrap8(s + k) for k in range(1, 8)]

    @pl.when(source)
    def _():
        first_sends.append(send(ew.at[:, pl.ds(half, 4096)], wpart, part_rs.at[0], partner, lambda: ew.at[:, 0:4096]))
        first_sends.append(send(vf.at[pl.ds(4 * (1 - c), 4)], vpart, part_rs.at[1], partner, lambda: vf.at[0:4]))
        first_sends.append(send(pixp, ppart, part_rs.at[2], partner, lambda: pixp))
        pltpu.make_async_copy(ew.at[:, pl.ds(pl.multiple_of(s * 1024, 1024), 1024)], eb.at[p, s], el_rs.at[s]).start()
        pltpu.make_async_copy(vf.at[s], vs.at[s], vl_rs.at[s]).start()
        pltpu.make_async_copy(pixt, px.at[p, s], pl_rs.at[s]).start()
        for sd in line_ids:
            col = pl.ds(pl.multiple_of(sd * 1024, 1024), 1024)
            first_sends.append(send(ew.at[:, col], eb.at[p, s], el_rs.at[s], dev(sd, p), lambda: ew.at[:, 0:1024]))
            first_sends.append(send(vf.at[sd], vs.at[s], vl_rs.at[s], dev(sd, p), lambda: vf.at[0]))
            first_sends.append(send(pixt, px.at[p, s], pl_rs.at[s], dev(sd, p), lambda: pixt))

    own_col = pl.ds(pl.multiple_of(s * 1024, 1024), 1024)
    pltpu.make_async_copy(vt_ref.at[:, own_col], vt.at[s], vt_rs.at[s]).start()
    for sd in line_ids:
        col = pl.ds(pl.multiple_of(sd * 1024, 1024), 1024)
        send(vt_ref.at[:, col], vt.at[s], vt_rs.at[s], dev(sd, p))

    kw_in.wait()
    lane = lax.broadcasted_iota(jnp.int32, (64, 128), 1)
    folded = jnp.where(lane < 64, lane, lane - 64)
    acc = jnp.zeros((64, 128), F32)
    for h in range(HEADS):
        cut = slice(h * HD, (h + 1) * HD)
        total = jnp.sum(kw[:, cut].astype(F32) * q_ref[:, cut], axis=1, keepdims=True)
        acc = jnp.where(folded == (h % 16) * 4 + h // 16, total, acc)
    high = acc.astype(BF).astype(F32)
    kqs[...] = jnp.where(lane < 64, high, acc - high).astype(BF)

    key_half = lax.rem(x, 2)
    key_core = lax.div(x, 2)
    key_sends = []
    for xd in range(3):
        target = dev(2 * xd + key_core, p)
        dst = kq.at[key_half, p, pl.ds(pl.multiple_of(c * 64, 64), 64), :]
        sem = kl_rs.at[key_half, c]

        away = target != me

        @pl.when(away)
        def _():
            key_sends.append((away, send(kqs, dst, sem, target, lambda: kqs)))

        @pl.when(target == me)
        def _():
            pltpu.make_async_copy(kqs, dst, sem).start()

    def place(oz, oy):
        return lax.rem(z + oz + 4, 4) * 4 + lax.rem(y + oy + 4, 4)

    def spread(dist, half_id, payloads, conditional=None):
        for o1 in OFFSETS:
            for o2 in OFFSETS:
                if abs(o1) + abs(o2) != dist:
                    continue
                oy, oz = (o1, o2) if half_id == 0 else (o2, o1)
                item = place(oz, oy)
                if dist > 0:
                    for ref_of, sems in payloads:
                        wait(ref_of(half_id, item), sems.at[half_id, item])
                sign = 1 if half_id == 0 else -1
                moves = []
                if o2 == 0:
                    if o1 == 0:
                        moves += [(1, 0), (-1, 0)]
                    elif o1 == -sign:
                        moves += [(sign, 0)]
                    moves += [(0, 1), (0, -1)]
                else:
                    f2 = sign if o1 in (0, 2) else -sign
                    if o2 == -f2:
                        moves += [(0, f2)]
                for m1, m2 in moves:
                    my, mz = (m1, m2) if half_id == 0 else (m2, m1)
                    target = dev(s, place(mz, my))
                    for ref_of, sems in payloads:
                        ref = ref_of(half_id, item)
                        if conditional is None:
                            send(ref, ref, sems.at[half_id, item], target)
                        else:
                            conditional.append(send(ref, ref, sems.at[half_id, item], target, lambda: ref_of(0, 0)))

    def key_block(half_id, item):
        return kq.at[half_id, item]

    def embed_block(half_id, item):
        return eb.at[item, pl.ds(0, 7), :, pl.ds(half_id * 512, 512)]

    def pixel_block(half_id, item):
        return px.at[item, :, :, pl.ds(half_id * 128, 128)]

    e_payloads = ((embed_block, eag_rs), (pixel_block, pag_rs))
    k_payloads = ((key_block, kag_rs),)
    k_sends = []

    def spread_keys(dist):
        @pl.when(source)
        def _():
            for half_id in (0, 1):
                spread(dist, half_id, k_payloads, k_sends)

    def spread_embed(dist):
        for half_id in (0, 1):
            spread(dist, half_id, e_payloads)

    @pl.when(source)
    def _():
        for a in range(2):
            for b in range(2):
                wait(kq.at[a, p, pl.ds(b * 64, 64), :], kl_rs.at[a, b])

    spread_keys(0)

    for u in range(6):
        wait(eb.at[p, u], el_rs.at[u])
        wait(vs.at[u], vl_rs.at[u])
        wait(px.at[p, u], pl_rs.at[u])
    row16 = lax.broadcasted_iota(jnp.int32, (16, 1024), 0)
    extra = jnp.zeros((16, 1024), F32)
    for u in range(6):
        extra = jnp.where(row16 == u, vs[u], extra)
    eb[p, 6] = extra.astype(BF)
    spread_embed(0)

    @pl.when(source)
    def _():
        wait(wpart, part_rs.at[0])
        wait(vpart, part_rs.at[1])
        wait(ppart, part_rs.at[2])
        own = pixp[...]
        other = ppart[...]
        for k in range(4):
            for n in range(2):
                lo = k * 1024 + n * 512
                w_own = jnp.where(c == 0, ew[:, lo : lo + 512], ew[:, 4096 + lo : 4096 + lo + 512])
                b_own = jnp.where(c == 0, vf[k, :, n * 512 : (n + 1) * 512], vf[4 + k, :, n * 512 : (n + 1) * 512])
                emb[0, :, lo : lo + 512] = (dot(own, w_own, ((1,), (0,))) + b_own).astype(BF)
                emb[1, :, lo : lo + 512] = (
                    dot(other, wpart[:, lo : lo + 512], ((1,), (0,))) + vpart[k, :, n * 512 : (n + 1) * 512]
                ).astype(BF)

    spread_keys(1)
    spread_keys(2)
    spread_embed(1)
    spread_keys(3)
    spread_keys(4)

    tail_sends = []

    @pl.when(source)
    def _():
        keys = kq[...].reshape(4096, 128)
        lps[...] = dot(emb[1], keys, ((1,), (0,)))
        tail_sends.append(send(lps, lpr, lp_rs.at[0], partner, lambda: lps))
        mine = dot(emb[0], keys, ((1,), (0,)))
        wait(lpr, lp_rs.at[0])
        turned = (mine + lpr[...]).T
        scaled = (turned[:64] + turned[64:]) / jnp.sqrt(jnp.float32(HD))
        for k in range(16):
            for n in range(2):
                ls[k, n * 4 : (n + 1) * 4, :] = scaled[4 * k : 4 * k + 4, n * 128 : (n + 1) * 128]
        pltpu.make_async_copy(ls.at[p], lq.at[p], lq_rs.at[0]).start()
        for k in range(1, 16):
            pd = wrap16(p + k)
            tail_sends.append(send(ls.at[pd], lq.at[p], lq_rs.at[0], dev(s, pd), lambda: ls.at[0]))

    spread_embed(2)

    @pl.when(source)
    def _():
        wait(lq, lq_rs.at[0])
        pltpu.make_async_copy(lq, lr.at[s], lr_rs.at[s]).start()
        for sd in line_ids:
            tail_sends.append(send(lq, lr.at[s], lr_rs.at[s], dev(sd, p), lambda: lq))

    pltpu.make_async_copy(ow_ref.at[:, own_col], ow.at[s], ow_rs.at[s]).start()
    for sd in line_ids:
        col = pl.ds(pl.multiple_of(sd * 1024, 1024), 1024)
        send(ow_ref.at[:, col], ow.at[s], ow_rs.at[s], dev(sd, p))

    for u in range(6):
        wait(lr.at[u], lr_rs.at[u])
    live = [(u, k) for u in range(6) for k in range(16) if (u // 2) * 32 + 2 * k + u % 2 < V]
    top = lr[0, 0]
    for u, k in live[1:]:
        top = jnp.maximum(top, lr[u, k])
    norm = jnp.zeros((8, 128), F32)
    for u, k in live:
        e = jnp.exp(lr[u, k] - top)
        aw[u, k] = e
        norm = norm + e
    for u in range(6):
        for k in range(16):
            if (u, k) in live:
                aw[u, k] = (aw[u, k] / norm).astype(BF).astype(F32)
            else:
                aw[u, k] = jnp.zeros((8, 128), F32)

    for k in range(8):
        wait(vt.at[k], vt_rs.at[k])
    row_n = lax.broadcasted_iota(jnp.int32, (16, 128), 0)

    def work(item):
        values = dot(vt[...].reshape(512, 1024), eb[item].reshape(128, 1024), ((1,), (1,)))
        evt[:, :, pl.ds(pl.multiple_of(item * 128, 128), 128)] = values.astype(BF).reshape(4, 128, 128)
        for n in range(2):
            lanes = slice(n * 128, (n + 1) * 128)
            tails = [jnp.zeros((16, 128), F32) for _ in range(4)]
            for u in range(6):
                pixel = px[item, u, :, lanes].astype(F32)
                weights = aw[u, item]
                for h in range(4):
                    w = weights[n * 4 + h : n * 4 + h + 1, :]
                    at[h, item, u * 16 : (u + 1) * 16, lanes] = (pixel * w).astype(BF)
                    tails[h] = jnp.where(row_n == u, w, tails[h])
            for h in range(4):
                at[h, item, 96:112, lanes] = tails[h].astype(BF)
                at[h, item, 112:128, lanes] = jnp.zeros((16, 128), BF)

    def work_all(dist):
        found = [(o1, o2) for o1 in OFFSETS for o2 in OFFSETS if abs(o1) + abs(o2) == dist]
        for o1, o2 in found:
            work(place(o1, o2))

    work_all(0)
    work_all(1)
    spread_embed(3)
    work_all(2)
    spread_embed(4)
    work_all(3)
    work_all(4)

    for k in range(1, 5):
        xd = lax.rem(x + k, 4)
        part = dot(evt[xd], at[xd].reshape(2048, 256), ((1,), (0,)))
        hp[2 * xd] = part[:64]
        hp[2 * xd + 1] = part[64:]
        if k < 4:
            for cd in range(2):
                send(hp.at[2 * xd + cd], hr.at[s], hr_rs.at[s], dev(2 * xd + cd, p))
        else:
            send(hp.at[2 * x + 1 - c], hr.at[s], hr_rs.at[s], partner)
    heads = hp[s]
    for sd in line_ids:
        wait(hr.at[sd], hr_rs.at[sd])
        heads = heads + hr[sd]
    hg[s] = heads.astype(BF)
    for sd in line_ids:
        send(hg.at[s], hg.at[s], hg_rs.at[s], dev(sd, p))
    for sd in line_ids:
        wait(hg.at[sd], hg_rs.at[sd])
    for k in range(8):
        wait(ow.at[k], ow_rs.at[k])

    mixed = dot(hg[...].reshape(512, 256), ow[...].reshape(512, 1024), ((0,), (0,)))
    ms[...] = mixed.astype(BF).reshape(16, 16, 1024)
    pltpu.make_async_copy(ms.at[p], mr.at[p], mr_rs.at[0]).start()
    for k in range(1, 16):
        pd = wrap16(p + k)
        send(ms.at[pd], mr.at[p], mr_rs.at[0], dev(s, pd))
    wait(mr, mr_rs.at[0])
    final = mr[0].astype(F32)
    for k in range(1, 16):
        final = final + mr[k].astype(F32)
    for k in range(8):
        ob[k] = final[2 * k : 2 * k + 2, :]
    pltpu.make_async_copy(ob.at[s], obr.at[s], ob_rs.at[s]).start()
    for sd in line_ids:
        send(ob.at[sd], obr.at[s], ob_rs.at[s], dev(sd, p))
    for k in range(8):
        wait(obr.at[k], ob_rs.at[k])
        out_ref[:, k * 1024 : (k + 1) * 1024] = obr[k].astype(BF)

    for ref, sem in pending:
        wait(ref, sem)
    for cond, pair in key_sends:

        @pl.when(cond)
        def _():
            drain([pair])

    @pl.when(source)
    def _():
        drain(first_sends)
        drain(k_sends)
        drain(tail_sends)


def body(pixels, embed_w, var_embed, key_w, query, value_t, out_w):
    vmem = pl.BlockSpec(memory_space=pltpu.VMEM)
    hbm = pl.BlockSpec(memory_space=pl.ANY)
    dma = pltpu.SemaphoreType.DMA
    return pl.pallas_call(
        kernel,
        out_shape=jax.ShapeDtypeStruct((2, D), BF),
        in_specs=[vmem, hbm, vmem, hbm, vmem, hbm, hbm],
        out_specs=vmem,
        scratch_shapes=[
            pltpu.VMEM((64, D), BF),
            pltpu.VMEM((16, D), BF),
            pltpu.VMEM((8, 1, 1024), F32),
            pltpu.VMEM((256, 16), BF),
            pltpu.VMEM((16, 256), BF),
            pltpu.VMEM((16, 4096), BF),
            pltpu.VMEM((4, 1, 1024), F32),
            pltpu.VMEM((256, 16), BF),
            pltpu.VMEM((2, 256, 4096), BF),
            pltpu.VMEM((64, 128), BF),
            pltpu.VMEM((2, 16, 128, 128), BF),
            pltpu.VMEM((16, 8, 16, 1024), BF),
            pltpu.VMEM((6, 1, 1024), F32),
            pltpu.VMEM((16, 6, 16, 256), BF),
            pltpu.VMEM((8, 64, 1024), BF),
            pltpu.VMEM((8, 64, 1024), BF),
            pltpu.VMEM((256, 128), F32),
            pltpu.VMEM((256, 128), F32),
            pltpu.VMEM((16, 8, 128), F32),
            pltpu.VMEM((16, 8, 128), F32),
            pltpu.VMEM((6, 16, 8, 128), F32),
            pltpu.VMEM((6, 16, 8, 128), F32),
            pltpu.VMEM((4, 128, 2048), BF),
            pltpu.VMEM((4, 16, 128, 256), BF),
            pltpu.VMEM((8, 64, 256), F32),
            pltpu.VMEM((8, 64, 256), F32),
            pltpu.VMEM((8, 64, 256), BF),
            pltpu.VMEM((16, 16, 1024), BF),
            pltpu.VMEM((16, 16, 1024), BF),
            pltpu.VMEM((8, 2, 1024), F32),
            pltpu.VMEM((8, 2, 1024), F32),
            dma((2,)),
            dma((220,)),
            dma((6,)),
            dma((6,)),
            dma((6,)),
            dma((3,)),
            dma((2, 2)),
            dma((8,)),
            dma((8,)),
            dma((2, 16)),
            dma((2, 16)),
            dma((2, 16)),
            dma((1,)),
            dma((1,)),
            dma((6,)),
            dma((8,)),
            dma((8,)),
            dma((1,)),
            dma((8,)),
        ],
        compiler_params=pltpu.CompilerParams(collective_id=0, has_side_effects=True, vmem_limit_bytes=56 * 1024 * 1024),
    )(pixels, embed_w, var_embed, key_w, query.reshape(1, D), value_t, out_w)


def solution(mesh):
    placed = (
        P("dev", None, None),
        P("dev", None, None),
        P("dev", None),
        P("dev", None),
        P(),
        P("dev", None),
        P("dev", None),
    )
    return jax.shard_map(body, mesh=mesh, in_specs=placed, out_specs=P("dev", None), check_vma=False)
```

```python
import jax
import jax.numpy as jnp
from jax import lax
from jax.experimental import pallas as pl
from jax.experimental.pallas import tpu as pltpu
from jax.sharding import PartitionSpec as P

D = 8192
HEADS = 64
HD = 128
V = 91
MESH = pl.DeviceIdType.MESH
BF = jnp.bfloat16
F32 = jnp.float32
OFFSETS = (0, -1, 1, 2)


def dot(a, b, dims):
    return lax.dot_general(a, b, (dims, ((), ())), preferred_element_type=F32)


def kernel(
    pix_ref,
    ew_ref,
    var_ref,
    kw_ref,
    q_ref,
    vt_ref,
    ow_ref,
    out_ref,
    q,
    pix,
    var,
    kw,
    ew,
    vf,
    pixp,
    pixt,
    wpart,
    vpart,
    ppart,
    emb,
    kqs,
    kq,
    eb,
    vs,
    px,
    vt,
    ow,
    lps,
    lpr,
    ls,
    lq,
    lr,
    aw,
    evt,
    at,
    hp,
    hr,
    hg,
    ms,
    mr,
    ob,
    loc_sem,
    ssem,
    el_rs,
    vl_rs,
    pl_rs,
    part_rs,
    kl_rs,
    vt_rs,
    ow_rs,
    kag_rs,
    eag_rs,
    pag_rs,
    pair_rs,
    lp_rs,
    lq_rs,
    lr_rs,
    hr_rs,
    hg_rs,
    mr_rs,
    ob_rs,
):
    me = lax.axis_index("dev")
    x = lax.div(me, 32)
    p = lax.rem(lax.div(me, 2), 16)
    c = lax.rem(me, 2)
    z = lax.div(p, 4)
    y = lax.rem(p, 4)
    s = 2 * x + c
    partner = x * 32 + p * 2 + (1 - c)
    source = x < 3

    def dev(s_, p_):
        return lax.div(s_, 2) * 32 + p_ * 2 + lax.rem(s_, 2)

    def wrap8(v):
        return lax.rem(v + 8, 8)

    def wrap16(v):
        return lax.rem(v + 16, 16)

    pending = []
    counter = [0]

    def send(src, dst, rs, d, like=None):
        number = counter[0]
        counter[0] += 1
        sem = ssem.at[0]
        pltpu.make_async_remote_copy(
            src_ref=src, dst_ref=dst, send_sem=sem, recv_sem=rs, device_id=(d,), device_id_type=MESH
        ).start()
        if like is None:
            pending.append((src, sem))
        return like, number

    def wait(ref, sem):
        pltpu.make_async_copy(ref, ref, sem).wait()

    def drain(pairs):
        for like, number in pairs:
            wait(like(), ssem.at[0])

    barrier = pltpu.get_barrier_semaphore()
    for k in range(1, 8):
        pl.semaphore_signal(barrier, inc=1, device_id=(dev(wrap8(s + k), p),), device_id_type=MESH)
    for k in range(1, 16):
        pl.semaphore_signal(barrier, inc=1, device_id=(dev(s, wrap16(p + k)),), device_id_type=MESH)
    loads = [
        pltpu.make_async_copy(src, dst, loc_sem.at[i])
        for i, (src, dst) in enumerate(
            ((q_ref, q), (kw_ref, kw), (pix_ref.at[0], pix), (var_ref, var), (ew_ref.at[0], ew))
        )
    ]
    for load in loads:
        load.start()

    pos = lax.broadcasted_iota(jnp.int32, (256, 256), 0)
    tok = lax.broadcasted_iota(jnp.int32, (256, 256), 1)
    want = lax.div(lax.rem(pos, 16), 4) * 64 + lax.div(pos, 16) * 4 + lax.rem(pos, 4)
    perm = jnp.where(tok == want, 1.0, 0.0).astype(BF)
    eb[:, 104:128, :] = jnp.zeros((16, 24, 1024), BF)

    loads[0].wait()
    loads[1].wait()
    lane = lax.broadcasted_iota(jnp.int32, (64, 128), 1)
    folded = jnp.where(lane < 64, lane, lane - 64)
    acc = jnp.zeros((64, 128), F32)
    for h in range(HEADS):
        cut = slice(h * HD, (h + 1) * HD)
        total = jnp.sum(kw[:, cut].astype(F32) * q[:, cut], axis=1, keepdims=True)
        acc = jnp.where(folded == (h % 16) * 4 + h // 16, total, acc)
    high = acc.astype(BF).astype(F32)
    kqs[...] = jnp.where(lane < 64, high, acc - high).astype(BF)

    loads[2].wait()
    pixt[...] = dot(pix[...], perm, ((1,), (1,))).astype(BF)
    pixp[...] = dot(perm, pix[...], ((1,), (1,))).astype(BF)
    loads[3].wait()
    for k in range(8):
        vf[k] = var[:, k * 1024 : (k + 1) * 1024].astype(F32)
    loads[4].wait()

    pl.semaphore_wait(barrier, 22)

    key_half = lax.rem(x, 2)
    key_core = lax.div(x, 2)
    key_sends = []
    for xd in range(3):
        target = dev(2 * xd + key_core, p)
        dst = kq.at[key_half, p, pl.ds(pl.multiple_of(c * 64, 64), 64), :]
        sem = kl_rs.at[key_half, c]
        away = target != me

        @pl.when(away)
        def _():
            key_sends.append((away, send(kqs, dst, sem, target, lambda: kqs)))

        @pl.when(target == me)
        def _():
            pltpu.make_async_copy(kqs, dst, sem).start()

    half = pl.multiple_of((1 - c) * 4096, 4096)
    first_sends = []
    line_ids = [wrap8(s + k) for k in range(1, 8)]

    @pl.when(source)
    def _():
        first_sends.append(send(ew.at[:, pl.ds(half, 4096)], wpart, part_rs.at[0], partner, lambda: ew.at[:, 0:4096]))
        first_sends.append(send(vf.at[pl.ds(4 * (1 - c), 4)], vpart, part_rs.at[1], partner, lambda: vf.at[0:4]))
        first_sends.append(send(pixp, ppart, part_rs.at[2], partner, lambda: pixp))
        row = pl.ds(pl.multiple_of(s * 16, 16), 16)
        pltpu.make_async_copy(
            ew.at[:, pl.ds(pl.multiple_of(s * 1024, 1024), 1024)], eb.at[p, row, :], el_rs.at[s]
        ).start()
        pltpu.make_async_copy(vf.at[s], vs.at[s], vl_rs.at[s]).start()
        own_lanes = pl.ds(pl.multiple_of(c * 128, 128), 128)
        pltpu.make_async_copy(pixt.at[:, own_lanes], px.at[p, s, :, own_lanes], pl_rs.at[s]).start()
        for sd in line_ids:
            col = pl.ds(pl.multiple_of(sd * 1024, 1024), 1024)
            lanes = pl.ds(pl.multiple_of(lax.rem(sd, 2) * 128, 128), 128)
            first_sends.append(
                send(ew.at[:, col], eb.at[p, row, :], el_rs.at[s], dev(sd, p), lambda: ew.at[:, 0:1024])
            )
            first_sends.append(send(vf.at[sd], vs.at[s], vl_rs.at[s], dev(sd, p), lambda: vf.at[0]))
            first_sends.append(
                send(pixt.at[:, lanes], px.at[p, s, :, lanes], pl_rs.at[s], dev(sd, p), lambda: pixt.at[:, 0:128])
            )

    own_col = pl.ds(pl.multiple_of(s * 1024, 1024), 1024)
    pltpu.make_async_copy(vt_ref.at[:, own_col], vt.at[s], vt_rs.at[s]).start()
    for sd in line_ids:
        col = pl.ds(pl.multiple_of(sd * 1024, 1024), 1024)
        send(vt_ref.at[:, col], vt.at[s], vt_rs.at[s], dev(sd, p))

    def place(oz, oy):
        return lax.rem(z + oz + 4, 4) * 4 + lax.rem(y + oy + 4, 4)

    def hand_over(half_id, item):
        ref = pixel_block(half_id, item)
        send(ref, ref, pair_rs.at[half_id, item], partner)

    def spread(dist, half_id, payloads, conditional=None):
        for o1 in OFFSETS:
            for o2 in OFFSETS:
                if abs(o1) + abs(o2) != dist:
                    continue
                oy, oz = (o1, o2) if half_id == 0 else (o2, o1)
                item = place(oz, oy)
                if dist > 0:
                    for ref_of, sems in payloads:
                        wait(ref_of(half_id, item), sems.at[half_id, item])
                if conditional is None:
                    hand_over(half_id, item)
                sign = 1 if half_id == 0 else -1
                moves = []
                if o2 == 0:
                    if o1 == 0:
                        moves += [(1, 0), (-1, 0)]
                    elif o1 == -sign:
                        moves += [(sign, 0)]
                    moves += [(0, 1), (0, -1)]
                else:
                    f2 = sign if o1 in (0, 2) else -sign
                    if o2 == -f2:
                        moves += [(0, f2)]
                for m1, m2 in moves:
                    my, mz = (m1, m2) if half_id == 0 else (m2, m1)
                    target = dev(s, place(mz, my))
                    for ref_of, sems in payloads:
                        ref = ref_of(half_id, item)
                        if conditional is None:
                            send(ref, ref, sems.at[half_id, item], target)
                        else:
                            conditional.append(send(ref, ref, sems.at[half_id, item], target, lambda: ref_of(0, 0)))

    def key_block(half_id, item):
        return kq.at[half_id, item]

    def embed_block(half_id, item):
        return eb.at[item, pl.ds(0, 104), pl.ds(half_id * 512, 512)]

    def pixel_block(half_id, item):
        return px.at[item, pl.ds(3 * half_id, 3), :, pl.ds(pl.multiple_of(c * 128, 128), 128)]

    e_payloads = ((embed_block, eag_rs), (pixel_block, pag_rs))
    k_payloads = ((key_block, kag_rs),)
    k_sends = []

    def spread_keys(dist):
        @pl.when(source)
        def _():
            for half_id in (0, 1):
                spread(dist, half_id, k_payloads, k_sends)

    def spread_embed(dist, half_id):
        spread(dist, half_id, e_payloads)

    @pl.when(source)
    def _():
        for a in range(2):
            for b in range(2):
                wait(kq.at[a, p, pl.ds(b * 64, 64), :], kl_rs.at[a, b])

    spread_keys(0)

    for u in range(6):
        wait(eb.at[p, u * 16 : (u + 1) * 16, :], el_rs.at[u])
        wait(vs.at[u], vl_rs.at[u])
        wait(px.at[p, u, :, pl.ds(pl.multiple_of(c * 128, 128), 128)], pl_rs.at[u])
    row8 = lax.broadcasted_iota(jnp.int32, (8, 1024), 0)
    extra = jnp.zeros((8, 1024), F32)
    for u in range(6):
        extra = jnp.where(row8 == u, vs[u], extra)
    eb[p, 96:104, :] = extra.astype(BF)
    spread_embed(0, 0)

    @pl.when(source)
    def _():
        wait(wpart, part_rs.at[0])
        wait(vpart, part_rs.at[1])
        wait(ppart, part_rs.at[2])
        own = pixp[...]
        other = ppart[...]
        for k in range(4):
            for n in range(2):
                lo = k * 1024 + n * 512
                w_own = jnp.where(c == 0, ew[:, lo : lo + 512], ew[:, 4096 + lo : 4096 + lo + 512])
                b_own = jnp.where(c == 0, vf[k, :, n * 512 : (n + 1) * 512], vf[4 + k, :, n * 512 : (n + 1) * 512])
                emb[0, :, lo : lo + 512] = (dot(own, w_own, ((1,), (0,))) + b_own).astype(BF)
                emb[1, :, lo : lo + 512] = (
                    dot(other, wpart[:, lo : lo + 512], ((1,), (0,))) + vpart[k, :, n * 512 : (n + 1) * 512]
                ).astype(BF)

    spread_keys(1)
    spread_embed(0, 1)
    spread_keys(2)
    spread_embed(1, 0)
    spread_keys(3)
    spread_embed(1, 1)
    spread_keys(4)

    tail_sends = []

    @pl.when(source)
    def _():
        keys = kq[...].reshape(4096, 128)
        lps[...] = dot(emb[1], keys, ((1,), (0,)))
        tail_sends.append(send(lps, lpr, lp_rs.at[0], partner, lambda: lps))
        mine = dot(emb[0], keys, ((1,), (0,)))
        wait(lpr, lp_rs.at[0])
        turned = (mine + lpr[...]).T
        scaled = (turned[:64] + turned[64:]) / jnp.sqrt(jnp.float32(HD))
        for k in range(16):
            for n in range(2):
                ls[k, n * 4 : (n + 1) * 4, :] = scaled[4 * k : 4 * k + 4, n * 128 : (n + 1) * 128]
        pltpu.make_async_copy(ls.at[p], lq.at[p], lq_rs.at[0]).start()
        for k in range(1, 16):
            pd = wrap16(p + k)
            tail_sends.append(send(ls.at[pd], lq.at[p], lq_rs.at[0], dev(s, pd), lambda: ls.at[0]))

    spread_embed(2, 0)
    spread_embed(2, 1)

    @pl.when(source)
    def _():
        wait(lq, lq_rs.at[0])
        pltpu.make_async_copy(lq, lr.at[s], lr_rs.at[s]).start()
        for sd in line_ids:
            tail_sends.append(send(lq, lr.at[s], lr_rs.at[s], dev(sd, p), lambda: lq))

    pltpu.make_async_copy(ow_ref.at[:, own_col], ow.at[s], ow_rs.at[s]).start()
    for sd in line_ids:
        col = pl.ds(pl.multiple_of(sd * 1024, 1024), 1024)
        send(ow_ref.at[:, col], ow.at[s], ow_rs.at[s], dev(sd, p))

    spread_embed(3, 0)
    spread_embed(3, 1)

    for k in range(8):
        wait(vt.at[k], vt_rs.at[k])

    def places(dist):
        return [place(o1, o2) for o1 in OFFSETS for o2 in OFFSETS if abs(o1) + abs(o2) == dist]

    def value_columns(dist):
        for item in places(dist):
            values = dot(vt[...].reshape(512, 1024), eb[item], ((1,), (1,)))
            evt[:, :, pl.ds(pl.multiple_of(item * 128, 128), 128)] = values.astype(BF).reshape(4, 128, 128)

    for dist in range(4):
        value_columns(dist)

    for u in range(6):
        wait(lr.at[u], lr_rs.at[u])
    live = [(u, k) for u in range(6) for k in range(16) if (u // 2) * 32 + 2 * k + u % 2 < V]
    top = lr[0, 0]
    for u, k in live[1:]:
        top = jnp.maximum(top, lr[u, k])
    norm = jnp.zeros((8, 128), F32)
    for u, k in live:
        e = jnp.exp(lr[u, k] - top)
        aw[u, k] = e
        norm = norm + e
    for u in range(6):
        for k in range(16):
            if (u, k) in live:
                aw[u, k] = (aw[u, k] / norm).astype(BF).astype(F32)
            else:
                aw[u, k] = jnp.zeros((8, 128), F32)

    row_n = lax.broadcasted_iota(jnp.int32, (16, 128), 0)

    def weigh(dist):
        for item in places(dist):
            other = pl.ds(pl.multiple_of((1 - c) * 128, 128), 128)
            for half_id in (0, 1):
                wait(px.at[item, pl.ds(3 * half_id, 3), :, other], pair_rs.at[half_id, item])
            for n in range(2):
                lanes = slice(n * 128, (n + 1) * 128)
                tails = [jnp.zeros((16, 128), F32) for _ in range(4)]
                for u in range(6):
                    pixel = px[item, u, :, lanes].astype(F32)
                    weights = aw[u, item]
                    for h in range(4):
                        w = weights[n * 4 + h : n * 4 + h + 1, :]
                        at[h, item, u * 16 : (u + 1) * 16, lanes] = (pixel * w).astype(BF)
                        tails[h] = jnp.where(row_n == u, w, tails[h])
                for h in range(4):
                    at[h, item, 96:112, lanes] = tails[h].astype(BF)
                    at[h, item, 112:128, lanes] = jnp.zeros((16, 128), BF)

    for dist in range(4):
        weigh(dist)
    spread_embed(4, 0)
    spread_embed(4, 1)
    value_columns(4)
    weigh(4)

    for k in range(1, 5):
        xd = lax.rem(x + k, 4)
        part = dot(evt[xd], at[xd].reshape(2048, 256), ((1,), (0,)))
        if k == 4:
            heads = jnp.where(c == 0, part[:64], part[64:])
        part = part.astype(BF)
        hp[2 * xd] = part[:64]
        hp[2 * xd + 1] = part[64:]
        if k < 4:
            for cd in range(2):
                send(hp.at[2 * xd + cd], hr.at[s], hr_rs.at[s], dev(2 * xd + cd, p))
        else:
            send(hp.at[2 * x + 1 - c], hr.at[s], hr_rs.at[s], partner)
    for sd in line_ids:
        wait(hr.at[sd], hr_rs.at[sd])
        heads = heads + hr[sd].astype(F32)
    hg[s] = heads.astype(BF)
    for sd in line_ids:
        send(hg.at[s], hg.at[s], hg_rs.at[s], dev(sd, p))
    for sd in line_ids:
        wait(hg.at[sd], hg_rs.at[sd])
    for k in range(8):
        wait(ow.at[k], ow_rs.at[k])

    mixed = dot(hg[...].reshape(512, 256), ow[...].reshape(512, 1024), ((0,), (0,)))
    ms[...] = mixed.astype(BF).reshape(16, 16, 1024)
    pltpu.make_async_copy(ms.at[p], mr.at[p], mr_rs.at[0]).start()
    for k in range(1, 16):
        pd = wrap16(p + k)
        send(ms.at[pd], mr.at[p], mr_rs.at[0], dev(s, pd))
    wait(mr, mr_rs.at[0])
    final = mr[0].astype(F32)
    for k in range(1, 16):
        final = final + mr[k].astype(F32)
    for k in range(8):
        ob[k] = final[2 * k : 2 * k + 2, :]
    pltpu.make_async_copy(ob.at[s], out_ref.at[s], ob_rs.at[s]).start()
    for sd in line_ids:
        send(ob.at[sd], out_ref.at[s], ob_rs.at[s], dev(sd, p))
    for k in range(8):
        wait(out_ref.at[k], ob_rs.at[k])

    for ref, sem in pending:
        wait(ref, sem)
    for cond, pair in key_sends:

        @pl.when(cond)
        def _():
            drain([pair])

    @pl.when(source)
    def _():
        drain(first_sends)
        drain(k_sends)
        drain(tail_sends)


def body(pixels, embed_w, var_embed, key_w, query, value_t, out_w):
    hbm = pl.BlockSpec(memory_space=pl.ANY)
    dma = pltpu.SemaphoreType.DMA
    slices = pl.pallas_call(
        kernel,
        out_shape=jax.ShapeDtypeStruct((8, 2, 1024), F32),
        in_specs=[hbm] * 7,
        out_specs=hbm,
        scratch_shapes=[
            pltpu.VMEM((1, D), F32),
            pltpu.VMEM((16, 256), BF),
            pltpu.VMEM((1, D), BF),
            pltpu.VMEM((64, D), BF),
            pltpu.VMEM((16, D), BF),
            pltpu.VMEM((8, 1, 1024), F32),
            pltpu.VMEM((256, 16), BF),
            pltpu.VMEM((16, 256), BF),
            pltpu.VMEM((16, 4096), BF),
            pltpu.VMEM((4, 1, 1024), F32),
            pltpu.VMEM((256, 16), BF),
            pltpu.VMEM((2, 256, 4096), BF),
            pltpu.VMEM((64, 128), BF),
            pltpu.VMEM((2, 16, 128, 128), BF),
            pltpu.VMEM((16, 128, 1024), BF),
            pltpu.VMEM((6, 1, 1024), F32),
            pltpu.VMEM((16, 6, 16, 256), BF),
            pltpu.VMEM((8, 64, 1024), BF),
            pltpu.VMEM((8, 64, 1024), BF),
            pltpu.VMEM((256, 128), F32),
            pltpu.VMEM((256, 128), F32),
            pltpu.VMEM((16, 8, 128), F32),
            pltpu.VMEM((16, 8, 128), F32),
            pltpu.VMEM((6, 16, 8, 128), F32),
            pltpu.VMEM((6, 16, 8, 128), F32),
            pltpu.VMEM((4, 128, 2048), BF),
            pltpu.VMEM((4, 16, 128, 256), BF),
            pltpu.VMEM((8, 64, 256), BF),
            pltpu.VMEM((8, 64, 256), BF),
            pltpu.VMEM((8, 64, 256), BF),
            pltpu.VMEM((16, 16, 1024), BF),
            pltpu.VMEM((16, 16, 1024), BF),
            pltpu.VMEM((8, 2, 1024), F32),
            dma((5,)),
            dma((1,)),
            dma((6,)),
            dma((6,)),
            dma((6,)),
            dma((3,)),
            dma((2, 2)),
            dma((8,)),
            dma((8,)),
            dma((2, 16)),
            dma((2, 16)),
            dma((2, 16)),
            dma((2, 16)),
            dma((1,)),
            dma((1,)),
            dma((6,)),
            dma((8,)),
            dma((8,)),
            dma((1,)),
            dma((8,)),
        ],
        compiler_params=pltpu.CompilerParams(collective_id=0, has_side_effects=True, vmem_limit_bytes=56 * 1024 * 1024),
    )(pixels.transpose(0, 2, 1), embed_w, var_embed, key_w, query.reshape(1, D), value_t, out_w)
    return slices.transpose(1, 0, 2).reshape(2, D).astype(BF)


def solution(mesh):
    placed = (
        P("dev", None, None),
        P("dev", None, None),
        P("dev", None),
        P("dev", None),
        P(),
        P("dev", None),
        P("dev", None),
    )
    return jax.shard_map(body, mesh=mesh, in_specs=placed, out_specs=P("dev", None), check_vma=False)
```

```python
import jax
import jax.numpy as jnp
from jax import lax
from jax.experimental import pallas as pl
from jax.experimental.pallas import tpu as pltpu
from jax.sharding import PartitionSpec as P

D = 8192
HEADS = 64
HD = 128
V = 91
MESH = pl.DeviceIdType.MESH
BF = jnp.bfloat16
F32 = jnp.float32
OFFSETS = (0, -1, 1, 2)


def dot(a, b, dims):
    return lax.dot_general(a, b, (dims, ((), ())), preferred_element_type=F32)


def kernel(
    pix_ref,
    ew_ref,
    var_ref,
    kw_ref,
    q_ref,
    vt_ref,
    ow_ref,
    out_ref,
    q,
    pix,
    var,
    kw,
    ew,
    vf,
    pixt,
    emb,
    kqs,
    kq,
    eb,
    vs,
    px,
    vt,
    ow,
    lp,
    lpr,
    ls,
    lr,
    aw,
    evt,
    at,
    hp,
    hr,
    hg,
    ms,
    mr,
    ob,
    loc_sem,
    ssem,
    el_rs,
    vl_rs,
    pl_rs,
    kq_rs,
    vt_rs,
    ow_rs,
    eag_rs,
    pag_rs,
    pair_rs,
    lp_rs,
    lr_rs,
    aw_rs,
    hr_rs,
    hg_rs,
    mr_rs,
    ob_rs,
):
    me = lax.axis_index("dev")
    x = lax.div(me, 32)
    p = lax.rem(lax.div(me, 2), 16)
    c = lax.rem(me, 2)
    z = lax.div(p, 4)
    y = lax.rem(p, 4)
    s = 2 * x + c
    partner = x * 32 + p * 2 + (1 - c)
    source = x < 3

    def dev(s_, p_):
        return lax.div(s_, 2) * 32 + p_ * 2 + lax.rem(s_, 2)

    def wrap8(v):
        return lax.rem(v + 8, 8)

    def wrap16(v):
        return lax.rem(v + 16, 16)

    pending = []
    counter = [0]

    def send(src, dst, rs, d, like=None):
        number = counter[0]
        counter[0] += 1
        sem = ssem.at[0]
        pltpu.make_async_remote_copy(
            src_ref=src, dst_ref=dst, send_sem=sem, recv_sem=rs, device_id=(d,), device_id_type=MESH
        ).start()
        if like is None:
            pending.append((src, sem))
        return like, number

    def wait(ref, sem):
        pltpu.make_async_copy(ref, ref, sem).wait()

    def drain(pairs):
        for like, number in pairs:
            wait(like(), ssem.at[0])

    barrier = pltpu.get_barrier_semaphore()
    for k in range(1, 8):
        pl.semaphore_signal(barrier, inc=1, device_id=(dev(wrap8(s + k), p),), device_id_type=MESH)
    for k in range(1, 16):
        for core in range(2):
            near = x * 32 + wrap16(p + k) * 2 + core
            pl.semaphore_signal(barrier, inc=1, device_id=(near,), device_id_type=MESH)
    loads = [
        pltpu.make_async_copy(src, dst, loc_sem.at[i])
        for i, (src, dst) in enumerate(
            ((q_ref, q), (kw_ref, kw), (pix_ref.at[0], pix), (var_ref, var), (ew_ref.at[0], ew))
        )
    ]
    for load in loads:
        load.start()

    pos = lax.broadcasted_iota(jnp.int32, (256, 256), 0)
    tok = lax.broadcasted_iota(jnp.int32, (256, 256), 1)
    want = lax.div(lax.rem(pos, 16), 4) * 64 + lax.div(pos, 16) * 4 + lax.rem(pos, 4)
    perm = jnp.where(tok == want, 1.0, 0.0).astype(BF)
    eb[:, 104:128, :] = jnp.zeros((16, 24, 1024), BF)
    ls[...] = jnp.zeros((16, 8, 128), F32)

    loads[0].wait()
    loads[1].wait()
    lane = lax.broadcasted_iota(jnp.int32, (64, 128), 1)
    folded = jnp.where(lane < 64, lane, lane - 64)
    acc = jnp.zeros((64, 128), F32)
    for h in range(HEADS):
        cut = slice(h * HD, (h + 1) * HD)
        total = jnp.sum(kw[:, cut].astype(F32) * q[:, cut], axis=1, keepdims=True)
        acc = jnp.where(folded == h, total, acc)
    high = acc.astype(BF).astype(F32)
    kqs[...] = jnp.where(lane < 64, high, acc - high).astype(BF)

    loads[2].wait()
    pixt[...] = dot(pix[...], perm, ((1,), (1,))).astype(BF)
    loads[3].wait()
    for k in range(8):
        vf[k] = var[:, k * 1024 : (k + 1) * 1024].astype(F32)
    loads[4].wait()

    pl.semaphore_wait(barrier, 37)

    key_core = lax.div(p, 8)
    key_dst = kq.at[lax.rem(p, 8) * 2 + c]
    at_home = key_core == c

    @pl.when(at_home)
    def _():
        pltpu.make_async_copy(kqs, key_dst, kq_rs.at[0]).start()

    across = []

    @pl.when(jnp.logical_not(at_home))
    def _():
        across.append(send(kqs, key_dst, kq_rs.at[0], partner, lambda: kqs))

    for k in range(1, 16):
        send(kqs, key_dst, kq_rs.at[0], x * 32 + wrap16(p + k) * 2 + key_core)

    first_sends = []
    line_ids = [wrap8(s + k) for k in range(1, 8)]

    @pl.when(source)
    def _():
        row = pl.ds(pl.multiple_of(s * 16, 16), 16)
        pltpu.make_async_copy(
            ew.at[:, pl.ds(pl.multiple_of(s * 1024, 1024), 1024)], eb.at[p, row, :], el_rs.at[s]
        ).start()
        pltpu.make_async_copy(vf.at[s], vs.at[s], vl_rs.at[s]).start()
        pltpu.make_async_copy(pixt, px.at[p, s], pl_rs.at[s]).start()
        for sd in line_ids:
            col = pl.ds(pl.multiple_of(sd * 1024, 1024), 1024)
            first_sends.append(
                send(ew.at[:, col], eb.at[p, row, :], el_rs.at[s], dev(sd, p), lambda: ew.at[:, 0:1024])
            )
            first_sends.append(send(vf.at[sd], vs.at[s], vl_rs.at[s], dev(sd, p), lambda: vf.at[0]))
            first_sends.append(send(pixt, px.at[p, s], pl_rs.at[s], dev(sd, p), lambda: pixt))

    own_col = pl.ds(pl.multiple_of(s * 1024, 1024), 1024)
    pltpu.make_async_copy(vt_ref.at[:, own_col], vt.at[s], vt_rs.at[s]).start()

    def hand_values(which):
        for sd in which:
            col = pl.ds(pl.multiple_of(sd * 1024, 1024), 1024)
            send(vt_ref.at[:, col], vt.at[s], vt_rs.at[s], dev(sd, p))

    def place(oz, oy):
        return lax.rem(z + oz + 4, 4) * 4 + lax.rem(y + oy + 4, 4)

    def hand_over(half_id, item):
        ref = pixel_block(half_id, item)
        send(ref, ref, pair_rs.at[half_id, item], partner)

    def spread_embed(dist, half_id):
        for o1 in OFFSETS:
            for o2 in OFFSETS:
                if abs(o1) + abs(o2) != dist:
                    continue
                oy, oz = (o1, o2) if half_id == 0 else (o2, o1)
                item = place(oz, oy)
                if dist > 0:
                    for ref_of, sems in e_payloads:
                        wait(ref_of(half_id, item), sems.at[half_id, item])
                    hand_over(half_id, item)
                sign = 1 if half_id == 0 else -1
                moves = []
                if o2 == 0:
                    if o1 == 0:
                        moves += [(1, 0), (-1, 0)]
                    elif o1 == -sign:
                        moves += [(sign, 0)]
                    moves += [(0, 1), (0, -1)]
                else:
                    f2 = sign if o1 in (0, 2) else -sign
                    if o2 == -f2:
                        moves += [(0, f2)]
                for m1, m2 in moves:
                    my, mz = (m1, m2) if half_id == 0 else (m2, m1)
                    target = dev(s, place(mz, my))
                    for ref_of, sems in e_payloads:
                        ref = ref_of(half_id, item)
                        send(ref, ref, sems.at[half_id, item], target)

    def embed_block(half_id, item):
        return eb.at[item, pl.ds(0, 104), pl.ds(half_id * 512, 512)]

    def pixel_block(half_id, item):
        return px.at[item, pl.ds(3 * half_id, 3), :, pl.ds(pl.multiple_of(c * 128, 128), 128)]

    e_payloads = ((embed_block, eag_rs), (pixel_block, pag_rs))

    for u in range(6):
        wait(eb.at[p, u * 16 : (u + 1) * 16, :], el_rs.at[u])
        wait(vs.at[u], vl_rs.at[u])
        wait(px.at[p, u], pl_rs.at[u])
    row8 = lax.broadcasted_iota(jnp.int32, (8, 1024), 0)
    extra = jnp.zeros((8, 1024), F32)
    for u in range(6):
        extra = jnp.where(row8 == u, vs[u], extra)
    eb[p, 96:104, :] = extra.astype(BF)
    spread_embed(0, 0)
    spread_embed(0, 1)
    hand_values(line_ids[:2])

    one = jnp.where(lax.broadcasted_iota(jnp.int32, (8, 256), 0) == 0, 1.0, 0.0).astype(BF)
    for u in range(6):
        first = jnp.where(row8 == 0, vs[u], 0.0).astype(BF)
        weights = jnp.concatenate([eb[p, u * 16 : (u + 1) * 16, :], first], axis=0)
        pixels = jnp.concatenate([px[p, u], one], axis=0)
        emb[u] = dot(weights, pixels, ((0,), (0,))).astype(BF)
    wait(kq, kq_rs.at[0])
    keys = kq[...].reshape(1024, 128).T
    for u in range(6):
        both = dot(keys, emb[u], ((1,), (0,)))
        both = both[:64] + both[64:]
        for k in range(8):
            h = k % 4
            lp[k, u] = both[h * 16 : (h + 1) * 16, (k // 4) * 128 : (k // 4 + 1) * 128]
    for sd in line_ids:
        send(lp.at[sd], lpr.at[s], lp_rs.at[s], dev(sd, p))

    spread_embed(1, 0)
    spread_embed(1, 1)

    logits = lp[s]
    for sd in line_ids:
        wait(lpr.at[sd], lp_rs.at[sd])
        logits = logits + lpr[sd]
    logits = logits / jnp.sqrt(jnp.float32(HD))
    for u in range(6):
        ls[:, u, :] = logits[u]
    pltpu.make_async_copy(ls.at[p], lr.at[p], lr_rs.at[0]).start()
    for k in range(1, 16):
        pd = wrap16(p + k)
        send(ls.at[pd], lr.at[p], lr_rs.at[0], dev(s, pd))
    hand_values(line_ids[2:])

    spread_embed(2, 0)
    spread_embed(2, 1)

    wait(lr, lr_rs.at[0])
    place_id = lax.broadcasted_iota(jnp.int32, (16, 8, 128), 0)
    slot_id = lax.broadcasted_iota(jnp.int32, (16, 8, 128), 1)
    variable = lax.div(slot_id, 2) * 32 + place_id * 2 + lax.rem(slot_id, 2)
    live = jnp.logical_and(slot_id < 6, variable < V)
    logits = jnp.where(live, lr[...], -1e30)
    top = jnp.max(jnp.max(logits, axis=0), axis=0, keepdims=True)
    weights = jnp.where(live, jnp.exp(logits - top), 0.0)
    norm = jnp.sum(jnp.sum(weights, axis=0), axis=0, keepdims=True)
    aw[s] = (weights / norm).astype(BF)
    for sd in line_ids:
        send(aw.at[s], aw.at[s], aw_rs.at[s], dev(sd, p))

    pltpu.make_async_copy(ow_ref.at[:, own_col], ow.at[s], ow_rs.at[s]).start()
    for sd in line_ids:
        col = pl.ds(pl.multiple_of(sd * 1024, 1024), 1024)
        send(ow_ref.at[:, col], ow.at[s], ow_rs.at[s], dev(sd, p))

    for k in range(8):
        wait(vt.at[k], vt_rs.at[k])

    def places(dist):
        return [place(o1, o2) for o1 in OFFSETS for o2 in OFFSETS if abs(o1) + abs(o2) == dist]

    def value_columns(dist):
        for item in places(dist):
            values = dot(vt[...].reshape(512, 1024), eb[item], ((1,), (1,)))
            evt[:, :, pl.ds(pl.multiple_of(item * 128, 128), 128)] = values.astype(BF).reshape(4, 128, 128)

    value_columns(0)
    value_columns(1)
    spread_embed(3, 0)
    spread_embed(3, 1)
    value_columns(2)
    value_columns(3)

    for sd in line_ids:
        wait(aw.at[sd], aw_rs.at[sd])

    row_n = lax.broadcasted_iota(jnp.int32, (16, 128), 0)

    def weigh(dist):
        for item in places(dist):
            other = pl.ds(pl.multiple_of((1 - c) * 128, 128), 128)
            for half_id in (0, 1):
                if dist > 0:
                    wait(px.at[item, pl.ds(3 * half_id, 3), :, other], pair_rs.at[half_id, item])
            for n in range(2):
                lanes = slice(n * 128, (n + 1) * 128)
                tails = [jnp.zeros((16, 128), F32) for _ in range(4)]
                tiles = [aw[n * 4 + h, item].astype(F32) for h in range(4)]
                for u in range(6):
                    pixel = px[item, u, :, lanes].astype(F32)
                    for h in range(4):
                        w = tiles[h][u : u + 1, :]
                        at[h, item, u * 16 : (u + 1) * 16, lanes] = (pixel * w).astype(BF)
                        tails[h] = jnp.where(row_n == u, w, tails[h])
                for h in range(4):
                    at[h, item, 96:112, lanes] = tails[h].astype(BF)
                    at[h, item, 112:128, lanes] = jnp.zeros((16, 128), BF)

    for dist in range(4):
        weigh(dist)
    spread_embed(4, 0)
    spread_embed(4, 1)
    value_columns(4)
    weigh(4)

    for k in range(1, 5):
        xd = lax.rem(x + k, 4)
        part = dot(evt[xd], at[xd].reshape(2048, 256), ((1,), (0,)))
        if k == 4:
            heads = jnp.where(c == 0, part[:64], part[64:])
        part = part.astype(BF)
        hp[2 * xd] = part[:64]
        hp[2 * xd + 1] = part[64:]
        if k < 4:
            for cd in range(2):
                send(hp.at[2 * xd + cd], hr.at[s], hr_rs.at[s], dev(2 * xd + cd, p))
        else:
            send(hp.at[2 * x + 1 - c], hr.at[s], hr_rs.at[s], partner)
    for sd in line_ids:
        wait(hr.at[sd], hr_rs.at[sd])
        heads = heads + hr[sd].astype(F32)
    hg[s] = heads.astype(BF)
    for sd in line_ids:
        send(hg.at[s], hg.at[s], hg_rs.at[s], dev(sd, p))
    for sd in line_ids:
        wait(hg.at[sd], hg_rs.at[sd])
    for k in range(8):
        wait(ow.at[k], ow_rs.at[k])

    mixed = dot(hg[...].reshape(512, 256), ow[...].reshape(512, 1024), ((0,), (0,)))
    ms[...] = mixed.astype(BF).reshape(16, 16, 1024)
    pltpu.make_async_copy(ms.at[p], mr.at[p], mr_rs.at[0]).start()
    for k in range(1, 16):
        pd = wrap16(p + k)
        send(ms.at[pd], mr.at[p], mr_rs.at[0], dev(s, pd))
    wait(mr, mr_rs.at[0])
    final = mr[0].astype(F32)
    for k in range(1, 16):
        final = final + mr[k].astype(F32)
    for k in range(8):
        ob[k] = final[2 * k : 2 * k + 2, :]
    pltpu.make_async_copy(ob.at[s], out_ref.at[s], ob_rs.at[s]).start()
    for sd in line_ids:
        send(ob.at[sd], out_ref.at[s], ob_rs.at[s], dev(sd, p))
    for k in range(8):
        wait(out_ref.at[k], ob_rs.at[k])

    for ref, sem in pending:
        wait(ref, sem)
    @pl.when(jnp.logical_not(at_home))
    def _():
        drain(across)

    @pl.when(source)
    def _():
        drain(first_sends)


def body(pixels, embed_w, var_embed, key_w, query, value_t, out_w):
    hbm = pl.BlockSpec(memory_space=pl.ANY)
    dma = pltpu.SemaphoreType.DMA
    slices = pl.pallas_call(
        kernel,
        out_shape=jax.ShapeDtypeStruct((8, 2, 1024), F32),
        in_specs=[hbm] * 7,
        out_specs=hbm,
        scratch_shapes=[
            pltpu.VMEM((1, D), F32),
            pltpu.VMEM((16, 256), BF),
            pltpu.VMEM((1, D), BF),
            pltpu.VMEM((64, D), BF),
            pltpu.VMEM((16, D), BF),
            pltpu.VMEM((8, 1, 1024), F32),
            pltpu.VMEM((16, 256), BF),
            pltpu.VMEM((6, 1024, 256), BF),
            pltpu.VMEM((64, 128), BF),
            pltpu.VMEM((16, 64, 128), BF),
            pltpu.VMEM((16, 128, 1024), BF),
            pltpu.VMEM((6, 1, 1024), F32),
            pltpu.VMEM((16, 6, 16, 256), BF),
            pltpu.VMEM((8, 64, 1024), BF),
            pltpu.VMEM((8, 64, 1024), BF),
            pltpu.VMEM((8, 6, 16, 128), F32),
            pltpu.VMEM((8, 6, 16, 128), F32),
            pltpu.VMEM((16, 8, 128), F32),
            pltpu.VMEM((16, 8, 128), F32),
            pltpu.VMEM((8, 16, 8, 128), BF),
            pltpu.VMEM((4, 128, 2048), BF),
            pltpu.VMEM((4, 16, 128, 256), BF),
            pltpu.VMEM((8, 64, 256), BF),
            pltpu.VMEM((8, 64, 256), BF),
            pltpu.VMEM((8, 64, 256), BF),
            pltpu.VMEM((16, 16, 1024), BF),
            pltpu.VMEM((16, 16, 1024), BF),
            pltpu.VMEM((8, 2, 1024), F32),
            dma((5,)),
            dma((1,)),
            dma((6,)),
            dma((6,)),
            dma((6,)),
            dma((1,)),
            dma((8,)),
            dma((8,)),
            dma((2, 16)),
            dma((2, 16)),
            dma((2, 16)),
            dma((8,)),
            dma((1,)),
            dma((8,)),
            dma((8,)),
            dma((8,)),
            dma((1,)),
            dma((8,)),
        ],
        compiler_params=pltpu.CompilerParams(collective_id=0, has_side_effects=True, vmem_limit_bytes=56 * 1024 * 1024),
    )(pixels.transpose(0, 2, 1), embed_w, var_embed, key_w, query.reshape(1, D), value_t, out_w)
    return slices.transpose(1, 0, 2).reshape(2, D).astype(BF)


def solution(mesh):
    placed = (
        P("dev", None, None),
        P("dev", None, None),
        P("dev", None),
        P("dev", None),
        P(),
        P("dev", None),
        P("dev", None),
    )
    return jax.shard_map(body, mesh=mesh, in_specs=placed, out_specs=P("dev", None), check_vma=False)
```
